128 devices in a mesh: member: 16 (over z, x_lo, core), space: 8 (over x_hi, y).
Axes of the slice: x: 4 (x_hi: 2, x_lo: 2; x = x_hi * 2 + x_lo), y: 4, z: 4, core: 2. Of those that a mesh axis runs over, the one named last changes fastest.
Arguments:
- weather: bfloat16 [16, 84, 256, 1440], P('member', None, 'space'), may hold values from -6 to 6
- coefficients: int32 [16, 84, 2, 368, 361], P('member', None, None, 'space'), may hold values from -1073741824 to 1073741823
- channel_scale: float32 [84], replicated, may hold values from 0.3 to 3
Outputs:
- perturbed: bfloat16 [16, 84, 256, 1440], P('member', None, 'space')
The draws below stay inside these ranges and needn't reach their ends.
All inputs are finite; a program needn't handle non-finite values.
Results may differ from the reference program's by a relative error of at most 0.007.
Values may be sent and summed in bfloat16 or wider, within the bound.
No kernel may reach another device: no remote copies, remote signals or barrier semaphores. Data moves between devices by JAX's collectives and lax.ppermute only.
A program may use at most 192 MiB of HBM per device.

```python
import math
import jax
import jax.numpy as jnp
from jax import lax

CH = 84
LON = 1440
E = 16
LAT = 256
LAT0 = 232
LP = 361
MP = 368


def with_ends(values, rng, low, largest):
    longest = values.shape.index(max(values.shape))
    spots = []
    for shift in (0, 1):
        where = [jax.random.randint(jax.random.fold_in(rng, axis), (), 0, length) for axis, length in enumerate(values.shape)]
        where[longest] = (where[longest] + shift) % values.shape[longest]
        spots.append(tuple(where))
    return values.at[spots[0]].set(low).at[spots[1]].set(largest)


def shard_levels(key, extent, pieces, least, high):
    level = 1.0
    for position, blocks in pieces:
        heights = jax.random.uniform(jax.random.fold_in(jax.random.fold_in(key, 6), position), (blocks,), jnp.float32, least / len(pieces), high / len(pieces))
        level = level * jnp.repeat(jnp.exp(heights), extent[position] // blocks).reshape((-1,) + (1,) * (len(extent) - 1 - position))
    return level


def normal_values(own_key, dims, spread, reach, shards=(), kind=jnp.bfloat16):
    loudness = shard_levels(own_key, dims, shards, -0.22, 0.18) if shards else 1.0
    values = jax.random.normal(own_key, dims, jnp.float32) * spread * loudness
    return jnp.minimum(jnp.maximum(values, -reach), reach).astype(kind)


def setup_inputs(seed: int = 0) -> dict:
    key_list = jax.random.split(jax.random.key(seed), 4)
    weather = normal_values(key_list[0], (E, CH, LAT, LON), 1.0, 6.0, ((0, 16), (2, 8)))
    coefficients = with_ends(jax.random.randint(key_list[1], (E, CH, 2, MP, LP), -1073741824, 1073741824), jax.random.fold_in(key_list[1], 1), -1073741824, 1073741823).astype(jnp.int32)
    channel_scale = jnp.clip(jnp.exp(jax.random.uniform(key_list[2], (CH,), jnp.float32, math.log(0.3), math.log(3.0))), 0.3, 3.0)
    return dict(weather=weather, coefficients=coefficients, channel_scale=channel_scale)


def diagonal_log(order_count):
    steps_up = jnp.arange(1, order_count, dtype=jnp.int32).astype(jnp.float32)
    terms = 0.5 * jnp.log((2.0 * steps_up + 1.0) / (2.0 * steps_up))
    return jnp.concatenate([jnp.zeros((1,), jnp.float32), jnp.cumsum(terms)])

def legendre_table(orders, colatitude, order_logs, degree_count):
    order_values = orders.astype(jnp.float32)[:, None]
    cosine = jnp.cos(colatitude)[None, :]
    sine_values = jnp.sin(colatitude)[None, :]
    diagonal = jnp.exp(order_logs[:, None] - 0.5 * math.log(4.0 * math.pi) + order_values * jnp.log(sine_values))
    block_size = 16
    turn_count = (degree_count + block_size - 1) // block_size
    order_square = order_values * order_values

    def advance(carry, turn_index):
        older_row, newer_row = carry
        produced = []
        for inner_step in range(block_size):
            degree = (turn_index * block_size + inner_step).astype(jnp.float32)
            degree_square = degree * degree
            prior = degree - 1.0
            factor_up = jnp.sqrt(jnp.maximum(4.0 * degree_square - 1.0, 1.0) / jnp.maximum(degree_square - order_square, 1.0))
            factor_down = jnp.sqrt(jnp.maximum(prior * prior - order_square, 0.0) / jnp.maximum(4.0 * prior * prior - 1.0, 1.0))
            next_row = factor_up * (cosine * newer_row - factor_down * older_row)
            next_row = jnp.where(degree < order_values, 0.0, jnp.where(degree == order_values, diagonal, next_row))
            produced.append(next_row)
            older_row, newer_row = (newer_row, next_row)
        return ((older_row, newer_row), jnp.stack(produced))
    empty = jnp.zeros_like(diagonal)
    carried, stacked = lax.scan(advance, (empty, empty), jnp.arange(turn_count, dtype=jnp.int32))
    return stacked.reshape(turn_count * block_size, orders.shape[0], colatitude.shape[0])[:degree_count]

def spectral_values(coefficients, orders):
    degree_count = coefficients.shape[-1]
    degrees = jnp.arange(degree_count, dtype=jnp.int32)
    keep = degrees[None, :] >= orders[:, None]
    factor = math.sqrt(3.0) * math.sqrt(4.0 * math.pi) / degree_count * 2.0 ** (-30)
    values = coefficients.astype(jnp.float32) * factor
    return jnp.where(keep, values, 0.0).astype(jnp.bfloat16)

def fourier_basis(order_count, lon_count):
    orders = jnp.arange(order_count, dtype=jnp.int32)
    columns = jnp.arange(lon_count, dtype=jnp.int32)
    phases = orders[:, None] * columns[None, :] % lon_count
    angles = 2.0 * math.pi / lon_count * phases.astype(jnp.float32)
    weights = jnp.where(orders == 0, 1.0, math.sqrt(2.0)).astype(jnp.float32)[:, None]
    return jnp.stack([weights * jnp.cos(angles), weights * jnp.sin(angles)]).astype(jnp.bfloat16)

def reference(weather, coefficients, channel_scale):
    orders = jnp.arange(MP, dtype=jnp.int32)
    colatitude = math.pi * (LAT0 + jnp.arange(LAT, dtype=jnp.int32)).astype(jnp.float32) / (LON // 2)
    legendre = legendre_table(orders, colatitude, diagonal_log(MP), LP).astype(jnp.bfloat16)
    legendre_wide = lax.optimization_barrier(legendre).astype(jnp.float32)
    basis = fourier_basis(MP, LON).reshape(2 * MP, LON)

    def one_member(coef_member):
        spectral = lax.optimization_barrier(spectral_values(coef_member, orders)).astype(jnp.float32)
        fourier = jnp.einsum('cpml,lmt->ctpm', spectral, legendre_wide, precision=lax.Precision.HIGHEST).astype(jnp.bfloat16)
        noise = jnp.dot(fourier.reshape(CH * LAT, 2 * MP), basis, preferred_element_type=jnp.float32)
        return noise.astype(jnp.bfloat16).reshape(CH, LAT, LON)
    noise_all = lax.map(one_member, coefficients)

    def add_up(total, noise_member):
        return (total + noise_member.astype(jnp.float32), None)
    total, unused = lax.scan(add_up, jnp.zeros((CH, LAT, LON), jnp.float32), noise_all)
    mean = total / E

    def perturb(pair):
        weather_member, noise_member = pair
        centred = noise_member.astype(jnp.float32) - mean
        return (weather_member.astype(jnp.float32) + channel_scale[:, None, None] * centred).astype(jnp.bfloat16)
    return lax.map(perturb, (weather, noise_all))
```

```python
import functools
import math

import jax
import jax.numpy as jnp
from jax import lax
from jax.experimental import pallas as pl
from jax.experimental.pallas import tpu as pltpu
from jax.sharding import PartitionSpec as P

F32 = jnp.float32
BF16 = jnp.bfloat16
SLOTS = 48
LEG_PITCH = 369
UNI_PITCH = 49
LEG_UNROLL = 8
VMEM = 60 * 2**20


def synthesis_kernel(first_ref, table_ref, coef_hbm, out_ref, coef, leg, uni, sem):
    channels, order_local, _, degree_count = coef.shape
    pairs = 2 * channels
    fetch = pltpu.make_async_copy(coef_hbm, coef, sem)
    fetch.start()
    order = lax.broadcasted_iota(jnp.int32, (SLOTS, 128), 0) + first_ref[0]
    order_square = order.astype(F32) * order.astype(F32)
    cosine = [jnp.broadcast_to(table_ref[0:1, 128 * h : 128 * h + 128], (SLOTS, 128)) for h in range(2)]
    diagonal = [table_ref[8 : 8 + SLOTS, 128 * h : 128 * h + 128] for h in range(2)]
    uni[0, 0:SLOTS, :] = jnp.zeros((SLOTS, 128), F32)
    empty = uni[0, 0:SLOTS, :]

    def advance(degree, carry):
        older, newer, down = carry
        value = jnp.full((8, 128), degree, jnp.int32).astype(F32)
        square = value * value
        inverse = 1.0 / (4.0 * square - 1.0)
        square = jnp.concatenate([square] * (SLOTS // 8))
        inverse = jnp.concatenate([inverse] * (SLOTS // 8))
        ratio = jnp.maximum((square - order_square) * inverse, 1e-30)
        up = lax.rsqrt(ratio)
        hit = order == degree
        made = []
        for h in range(2):
            row = jnp.where(hit, diagonal[h], up * (cosine[h] * newer[h] - down * older[h]))
            leg[h, pl.ds(degree, SLOTS, stride=LEG_PITCH), :] = row
            made.append(row)
        return newer, tuple(made), ratio * up

    def advance_some(turn, carry):
        for u in range(LEG_UNROLL):
            carry = advance(turn * LEG_UNROLL + u, carry)
        return carry

    lax.fori_loop(0, -(-degree_count // LEG_UNROLL), advance_some, ((empty, empty), (empty, empty), empty))
    fetch.wait()
    factor = math.sqrt(3.0) * math.sqrt(4.0 * math.pi) / degree_count * 2.0 ** (-30)

    def sum_degrees(m):
        spectral = (coef[:, m, :, :].astype(F32) * factor).reshape(pairs, degree_count).astype(BF16)
        for h in range(2):
            legendre = leg[h, pl.ds(m * LEG_PITCH, degree_count), :].astype(BF16)
            fourier = jnp.dot(spectral, legendre, preferred_element_type=F32)
            uni[h, pl.ds(m, pairs, stride=UNI_PITCH), :] = fourier

    def sum_two(turn, carry):
        sum_degrees(2 * turn)
        sum_degrees(2 * turn + 1)
        return carry

    lax.fori_loop(0, order_local // 2, sum_two, 0)
    blank = jnp.zeros((pairs, 128), F32)
    for h in range(2):
        for m in range(order_local, SLOTS):
            uni[h, pl.ds(m, pairs, stride=UNI_PITCH), :] = blank
    lane_group = lax.broadcasted_iota(jnp.int32, (2 * SLOTS, 128), 1) // 32

    def regroup(q, carry):
        for h in range(2):
            parts = [
                jnp.concatenate([uni[h, pl.ds((8 * q + 2 * i + p) * UNI_PITCH, SLOTS), :] for p in range(2)])
                for i in range(4)
            ]
            for group in range(4):
                joined = None
                for i in range(4):
                    turn = (i - group) % 4
                    moved = parts[i] if turn == 0 else pltpu.roll(parts[i], 32 * turn, 1)
                    joined = moved if joined is None else jnp.where(lane_group == i, moved, joined)
                joined = joined.astype(BF16)
                for j in range(3):
                    t = 3 * q + j
                    row = pl.multiple_of(32 * (t % 4), 32)
                    out_ref[t // 4, 4 * h + group, pl.ds(row, 32), :] = joined[32 * j : 32 * j + 32]
        return carry

    lax.fori_loop(0, channels // 4, regroup, 0)
    for s in range(8):
        out_ref[15, s, 96:128, :] = jnp.zeros((32, 128), BF16)


def centre_kernel(in_ref, out_ref):
    members = in_ref.shape[0]
    total = in_ref[0, 0].astype(F32)
    for e in range(1, members):
        total = total + in_ref[e, 0].astype(F32)
    mean = total * (1.0 / members)
    for e in range(members):
        out_ref[e, 0] = (in_ref[e, 0].astype(F32) - mean).astype(BF16)


def perturb_kernel(groups, scale_ref, rows_ref, basis_ref, weather_ref, out_ref):
    step = pl.program_id(0)
    columns = []
    for g in range(groups):
        pieces = []
        for s in range(8):
            for j in range(3):
                t = 3 * (step * groups + g) + j
                pieces.append(rows_ref[t // 4, s, pl.ds(pl.multiple_of(32 * (t % 4), 32), 32), :])
        columns.append(jnp.concatenate(pieces, axis=0))
    noise = lax.dot_general(
        jnp.concatenate(columns, axis=1), basis_ref[...], (((0,), (0,)), ((), ())), preferred_element_type=F32
    )
    for c in range(4 * groups):
        scale = scale_ref[step * 4 * groups + c]
        out_ref[c] = (weather_ref[c].astype(F32) + scale * noise[32 * c : 32 * c + 32]).astype(BF16)


def legendre_start(first_order, colatitude):
    orders = first_order + jnp.arange(SLOTS, dtype=jnp.int32)
    steps = jnp.arange(1, 384, dtype=jnp.int32)
    terms = 0.5 * jnp.log((2.0 * steps.astype(F32) + 1.0) / (2.0 * steps.astype(F32)))
    logs = jnp.sum(jnp.where(steps[None, :] <= orders[:, None], terms[None, :], 0.0), axis=1)
    diagonal = jnp.exp(
        logs[:, None]
        - 0.5 * math.log(4.0 * math.pi)
        + orders.astype(F32)[:, None] * jnp.log(jnp.sin(colatitude))[None, :]
    )
    cosine = jnp.broadcast_to(jnp.cos(colatitude)[None, :], (8, colatitude.shape[0]))
    return jnp.concatenate([cosine, diagonal])


def fourier_basis(bands, order_local, lon_count):
    slots = jnp.arange(SLOTS, dtype=jnp.int32)
    orders = order_local * jnp.arange(bands, dtype=jnp.int32)[:, None] + slots[None, :]
    columns = jnp.arange(lon_count, dtype=jnp.int32)
    phases = orders[:, :, None] * columns % lon_count
    angles = 2.0 * math.pi / lon_count * phases.astype(F32)
    weights = jnp.where(orders == 0, 1.0, math.sqrt(2.0))
    weights = jnp.where(slots[None, :] < order_local, weights, 0.0).astype(F32)[:, :, None]
    both = jnp.stack([weights * jnp.cos(angles), weights * jnp.sin(angles)], axis=1)
    return both.astype(BF16).reshape(bands * 2 * SLOTS, lon_count)


def local(weather, coefficients, channel_scale):
    members = lax.axis_size("member")
    bands = lax.axis_size("space")
    _, channels, rows_local, lon_count = weather.shape
    order_local, degree_count = coefficients.shape[3:]
    lat_count = rows_local * bands
    first_order = lax.axis_index("space") * order_local
    row_first = (lon_count // 2 + 1 - lat_count) // 2
    colatitude = math.pi * (row_first + jnp.arange(lat_count, dtype=jnp.int32)).astype(F32) / (lon_count // 2)
    vmem = pl.BlockSpec(memory_space=pltpu.VMEM)
    smem = pl.BlockSpec(memory_space=pltpu.SMEM)
    params = pltpu.CompilerParams(vmem_limit_bytes=VMEM)
    block = (members, bands, 128, 128)

    coef = jnp.transpose(coefficients[0], (0, 2, 1, 3))
    fourier = pl.pallas_call(
        synthesis_kernel,
        in_specs=[smem, vmem, pl.BlockSpec(memory_space=pl.ANY)],
        out_specs=vmem,
        out_shape=jax.ShapeDtypeStruct(block, BF16),
        scratch_shapes=[
            pltpu.VMEM((channels, order_local, 2, degree_count), jnp.int32),
            pltpu.VMEM((2, SLOTS * LEG_PITCH + 8, 128), F32),
            pltpu.VMEM((2, 2 * channels * UNI_PITCH, 128), F32),
            pltpu.SemaphoreType.DMA,
        ],
        compiler_params=params,
        name="synthesis",
    )(first_order.reshape(1), legendre_start(first_order, colatitude), coef)

    owned = lax.all_to_all(
        fourier.reshape(members * bands, 128, 128), ("member", "space"), split_axis=0, concat_axis=0, tiled=True
    )
    spec = pl.BlockSpec((members, 1, 128, 128), lambda s: (0, s, 0, 0))
    centred = pl.pallas_call(
        centre_kernel,
        grid=(bands,),
        in_specs=[spec],
        out_specs=spec,
        out_shape=jax.ShapeDtypeStruct(block, BF16),
        compiler_params=params,
        name="centre",
    )(owned.reshape(block))
    rows = lax.all_to_all(centred, "member", split_axis=0, concat_axis=0, tiled=True)

    groups = 7
    band = pl.BlockSpec((4 * groups, rows_local, lon_count), lambda i: (i, 0, 0))
    basis = fourier_basis(bands, order_local, lon_count)
    perturbed = pl.pallas_call(
        functools.partial(perturb_kernel, groups),
        grid=(channels // (4 * groups),),
        in_specs=[
            smem,
            pl.BlockSpec(block, lambda i: (0, 0, 0, 0)),
            pl.BlockSpec(basis.shape, lambda i: (0, 0)),
            band,
        ],
        out_specs=band,
        out_shape=jax.ShapeDtypeStruct(weather.shape[1:], BF16),
        compiler_params=params,
        name="perturb",
    )(channel_scale, rows, basis, weather[0])
    return perturbed[None]


def solution(mesh):
    return jax.shard_map(
        local,
        mesh=mesh,
        in_specs=(P("member", None, "space", None), P("member", None, None, "space", None), P()),
        out_specs=P("member", None, "space", None),
        check_vma=False,
    )
```

```python
import functools
import math

import jax
import jax.numpy as jnp
from jax import lax
from jax.experimental import pallas as pl
from jax.experimental.pallas import tpu as pltpu
from jax.sharding import PartitionSpec as P

F32 = jnp.float32
BF16 = jnp.bfloat16
SLOTS = 48
LEG_PITCH = 369
UNI_PITCH = 49
LEG_UNROLL = 8
VMEM = 60 * 2**20


def relative_part(part, me):
    return ((part ^ me) & 1) * 8 + ((part // 4 - me // 4) & 3) * 2 + (((part ^ me) // 2) & 1)


def synthesis_kernel(first_ref, table_ref, coef_hbm, out_ref, coef, leg, uni, sem):
    channels, order_local, _, degree_count = coef.shape
    pairs = 2 * channels
    fetch = pltpu.make_async_copy(coef_hbm, coef, sem)
    fetch.start()
    me = first_ref[1]
    order = lax.broadcasted_iota(jnp.int32, (SLOTS, 128), 0) + first_ref[0]
    order_square = order.astype(F32) * order.astype(F32)
    cosine = [jnp.broadcast_to(table_ref[0:1, 128 * h : 128 * h + 128], (SLOTS, 128)) for h in range(2)]
    diagonal = [table_ref[8 : 8 + SLOTS, 128 * h : 128 * h + 128] for h in range(2)]
    uni[0, 0:SLOTS, :] = jnp.zeros((SLOTS, 128), F32)
    empty = uni[0, 0:SLOTS, :]

    def advance(degree, carry):
        older, newer, down = carry
        value = jnp.full((8, 128), degree, jnp.int32).astype(F32)
        square = value * value
        inverse = 1.0 / (4.0 * square - 1.0)
        square = jnp.concatenate([square] * (SLOTS // 8))
        inverse = jnp.concatenate([inverse] * (SLOTS // 8))
        ratio = jnp.maximum((square - order_square) * inverse, 1e-30)
        up = lax.rsqrt(ratio)
        hit = order == degree
        made = []
        for h in range(2):
            row = jnp.where(hit, diagonal[h], up * (cosine[h] * newer[h] - down * older[h]))
            leg[h, pl.ds(degree, SLOTS, stride=LEG_PITCH), :] = row
            made.append(row)
        return newer, tuple(made), ratio * up

    def advance_some(turn, carry):
        for u in range(LEG_UNROLL):
            carry = advance(turn * LEG_UNROLL + u, carry)
        return carry

    lax.fori_loop(0, -(-degree_count // LEG_UNROLL), advance_some, ((empty, empty), (empty, empty), empty))
    fetch.wait()
    factor = math.sqrt(3.0) * math.sqrt(4.0 * math.pi) / degree_count * 2.0 ** (-30)

    def sum_degrees(m):
        spectral = (coef[:, m, :, :].astype(F32) * factor).reshape(pairs, degree_count).astype(BF16)
        for h in range(2):
            legendre = leg[h, pl.ds(m * LEG_PITCH, degree_count), :].astype(BF16)
            fourier = jnp.dot(spectral, legendre, preferred_element_type=F32)
            uni[h, pl.ds(m, pairs, stride=UNI_PITCH), :] = fourier

    def sum_two(turn, carry):
        sum_degrees(2 * turn)
        sum_degrees(2 * turn + 1)
        return carry

    lax.fori_loop(0, order_local // 2, sum_two, 0)
    blank = jnp.zeros((pairs, 128), F32)
    for h in range(2):
        for m in range(order_local, SLOTS):
            uni[h, pl.ds(m, pairs, stride=UNI_PITCH), :] = blank
    lane_group = lax.broadcasted_iota(jnp.int32, (2 * SLOTS, 128), 1) // 32

    def regroup(q, carry):
        for h in range(2):
            parts = [
                jnp.concatenate([uni[h, pl.ds((8 * q + 2 * i + p) * UNI_PITCH, SLOTS), :] for p in range(2)])
                for i in range(4)
            ]
            for group in range(4):
                joined = None
                for i in range(4):
                    turn = (i - group) % 4
                    moved = parts[i] if turn == 0 else pltpu.roll(parts[i], 32 * turn, 1)
                    joined = moved if joined is None else jnp.where(lane_group == i, moved, joined)
                joined = joined.astype(BF16)
                for j in range(3):
                    t = 3 * q + j
                    row = pl.multiple_of(32 * (t % 4), 32)
                    out_ref[4 * h + group, relative_part(t // 4, me), pl.ds(row, 32), :] = joined[32 * j : 32 * j + 32]
        return carry

    lax.fori_loop(0, channels // 4, regroup, 0)
    for s in range(8):
        out_ref[s, relative_part(15, me), 96:128, :] = jnp.zeros((32, 128), BF16)


def pair_kernel(own_ref, other_ref, *out_refs):
    for dz, out_ref in enumerate(out_refs):
        for dx in range(2):
            i = 2 * dz + dx
            out_ref[0, dx] = (own_ref[0, i].astype(F32) + other_ref[0, i].astype(F32)).astype(BF16)


def column_kernel(a_ref, b_ref, c_ref, d_ref, stay_ref, give_ref):
    for dx, out_ref in enumerate((stay_ref, give_ref)):
        total = a_ref[0, dx].astype(F32) + b_ref[0, dx].astype(F32)
        total = total + c_ref[0, dx].astype(F32) + d_ref[0, dx].astype(F32)
        out_ref[0] = total.astype(BF16)


def mean_kernel(stay_ref, got_ref, out_ref):
    total = stay_ref[0].astype(F32) + got_ref[0].astype(F32)
    out_ref[0] = (total * (1.0 / 16.0)).astype(BF16)


def perturb_kernel(groups, scale_ref, me_ref, basis_ref, weather_ref, rows_ref, *refs):
    mean_refs, out_ref, centred = refs[:8], refs[8], refs[9]
    step = pl.program_id(0)
    me = me_ref[1]

    @pl.when(step == 0)
    def _():
        for k, mean_ref in enumerate(mean_refs):
            for dx in range(2):
                for s in range(8):
                    value = rows_ref[s, 2 * k + dx].astype(F32) - mean_ref[dx, s].astype(F32)
                    centred[s, 2 * k + dx] = value.astype(BF16)

    columns = []
    for g in range(groups):
        pieces = []
        for s in range(8):
            for j in range(3):
                t = 3 * (step * groups + g) + j
                part = relative_part(t // 4, me)
                pieces.append(centred[s, part, pl.ds(pl.multiple_of(32 * (t % 4), 32), 32), :])
        columns.append(jnp.concatenate(pieces, axis=0))
    noise = lax.dot_general(
        jnp.concatenate(columns, axis=1), basis_ref[...], (((0,), (0,)), ((), ())), preferred_element_type=F32
    )
    for c in range(4 * groups):
        scale = scale_ref[step * 4 * groups + c]
        out_ref[c] = (weather_ref[c].astype(F32) + scale * noise[32 * c : 32 * c + 32]).astype(BF16)


def legendre_start(first_order, colatitude):
    orders = first_order + jnp.arange(SLOTS, dtype=jnp.int32)
    steps = jnp.arange(1, 384, dtype=jnp.int32)
    terms = 0.5 * jnp.log((2.0 * steps.astype(F32) + 1.0) / (2.0 * steps.astype(F32)))
    logs = jnp.sum(jnp.where(steps[None, :] <= orders[:, None], terms[None, :], 0.0), axis=1)
    diagonal = jnp.exp(
        logs[:, None]
        - 0.5 * math.log(4.0 * math.pi)
        + orders.astype(F32)[:, None] * jnp.log(jnp.sin(colatitude))[None, :]
    )
    cosine = jnp.broadcast_to(jnp.cos(colatitude)[None, :], (8, colatitude.shape[0]))
    return jnp.concatenate([cosine, diagonal])


def fourier_basis(bands, order_local, lon_count):
    slots = jnp.arange(SLOTS, dtype=jnp.int32)
    orders = order_local * jnp.arange(bands, dtype=jnp.int32)[:, None] + slots[None, :]
    columns = jnp.arange(lon_count, dtype=jnp.int32)
    phases = orders[:, :, None] * columns % lon_count
    angles = 2.0 * math.pi / lon_count * phases.astype(F32)
    weights = jnp.where(orders == 0, 1.0, math.sqrt(2.0))
    weights = jnp.where(slots[None, :] < order_local, weights, 0.0).astype(F32)[:, :, None]
    both = jnp.stack([weights * jnp.cos(angles), weights * jnp.sin(angles)], axis=1)
    return both.astype(BF16).reshape(bands * 2 * SLOTS, lon_count)


def local(weather, coefficients, channel_scale):
    members = lax.axis_size("member")
    bands = lax.axis_size("space")
    _, channels, rows_local, lon_count = weather.shape
    order_local, degree_count = coefficients.shape[3:]
    lat_count = rows_local * bands
    first_order = lax.axis_index("space") * order_local
    row_first = (lon_count // 2 + 1 - lat_count) // 2
    colatitude = math.pi * (row_first + jnp.arange(lat_count, dtype=jnp.int32)).astype(F32) / (lon_count // 2)
    vmem = pl.BlockSpec(memory_space=pltpu.VMEM)
    smem = pl.BlockSpec(memory_space=pltpu.SMEM)
    params = pltpu.CompilerParams(vmem_limit_bytes=VMEM)
    me = lax.axis_index("member")
    place = jnp.stack([first_order, me])
    block = (bands, members, 128, 128)
    ring = range(members)

    def to_core(x):
        return lax.ppermute(x, "member", [(e, e ^ 1) for e in ring])

    def to_chip(x):
        return lax.ppermute(x, "member", [(e, e ^ 2) for e in ring])

    def along_z(x, steps):
        return lax.ppermute(x, "member", [(e, (e + 4 * steps) % members) for e in ring])

    def by_band(parts):
        lead = () if parts == 1 else (parts,)
        return pl.BlockSpec((1, *lead, 128, 128), lambda s: (s,) + (0,) * (len(lead) + 2))

    def like(parts):
        lead = () if parts == 1 else (parts,)
        return jax.ShapeDtypeStruct((bands, *lead, 128, 128), BF16)

    coef = jnp.transpose(coefficients[0], (0, 2, 1, 3))
    fourier = pl.pallas_call(
        synthesis_kernel,
        in_specs=[smem, vmem, pl.BlockSpec(memory_space=pl.ANY)],
        out_specs=vmem,
        out_shape=jax.ShapeDtypeStruct(block, BF16),
        scratch_shapes=[
            pltpu.VMEM((channels, order_local, 2, degree_count), jnp.int32),
            pltpu.VMEM((2, SLOTS * LEG_PITCH + 8, 128), F32),
            pltpu.VMEM((2, 2 * channels * UNI_PITCH, 128), F32),
            pltpu.SemaphoreType.DMA,
        ],
        compiler_params=params,
        name="synthesis",
    )(place, legendre_start(first_order, colatitude), coef)

    rows = lax.all_to_all(fourier, "space", split_axis=0, concat_axis=0, tiled=True)
    got = to_core(fourier[:, 8:])
    sums = pl.pallas_call(
        pair_kernel,
        grid=(bands,),
        in_specs=[by_band(8), by_band(8)],
        out_specs=[by_band(2)] * 4,
        out_shape=[like(2)] * 4,
        name="pair_sum",
    )(fourier, got)
    arrived = [along_z(sums[d], d) for d in (1, 2, 3)]
    stay, give = pl.pallas_call(
        column_kernel,
        grid=(bands,),
        in_specs=[by_band(2)] * 4,
        out_specs=[by_band(1)] * 2,
        out_shape=[like(1)] * 2,
        name="column_sum",
    )(sums[0], *arrived)
    given = to_chip(give)
    mean = pl.pallas_call(
        mean_kernel,
        grid=(bands,),
        in_specs=[by_band(1)] * 2,
        out_specs=by_band(1),
        out_shape=like(1),
        name="mean",
    )(stay, given)
    mean, rows = lax.optimization_barrier((mean, rows))
    mean = lax.all_to_all(mean, "space", split_axis=0, concat_axis=0, tiled=True)
    both = jnp.stack([mean, to_chip(mean)])
    tower = [both] + [along_z(both, 4 - d) for d in (1, 2, 3)]
    means = tower + [to_core(x) for x in tower]

    groups = 7
    band = pl.BlockSpec((4 * groups, rows_local, lon_count), lambda i: (i, 0, 0))
    basis = fourier_basis(bands, order_local, lon_count)
    perturbed = pl.pallas_call(
        functools.partial(perturb_kernel, groups),
        grid=(channels // (4 * groups),),
        in_specs=[
            smem,
            smem,
            pl.BlockSpec(basis.shape, lambda i: (0, 0)),
            band,
            pl.BlockSpec(block, lambda i: (0, 0, 0, 0)),
        ]
        + [pl.BlockSpec((2, bands, 128, 128), lambda i: (0, 0, 0, 0))] * 8,
        out_specs=band,
        out_shape=jax.ShapeDtypeStruct(weather.shape[1:], BF16),
        scratch_shapes=[pltpu.VMEM(block, BF16)],
        compiler_params=params,
        name="perturb",
    )(channel_scale, place, basis, weather[0], rows, *means)
    return perturbed[None]


def solution(mesh):
    return jax.shard_map(
        local,
        mesh=mesh,
        in_specs=(P("member", None, "space", None), P("member", None, None, "space", None), P()),
        out_specs=P("member", None, "space", None),
        check_vma=False,
    )
```

```python
import functools
import math

import jax
import jax.numpy as jnp
from jax import lax
from jax.experimental import pallas as pl
from jax.experimental.pallas import tpu as pltpu
from jax.sharding import PartitionSpec as P

F32 = jnp.float32
BF16 = jnp.bfloat16
SLOTS = 48
LEG_PITCH = 369
UNI_PITCH = 49
LEG_UNROLL = 8
VMEM = 60 * 2**20


def relative_part(part, me):
    return ((part ^ me) & 1) * 8 + ((part // 4 - me // 4) & 3) * 2 + (((part ^ me) // 2) & 1)


def synthesis_kernel(first_ref, table_ref, coef_hbm, keep_hbm, away_hbm, coef, leg, uni, out_ref, sems):
    channels, order_local, _, degree_count = coef.shape
    pairs = 2 * channels
    fetch = pltpu.make_async_copy(coef_hbm, coef, sems.at[0])
    fetch.start()
    me = first_ref[1]
    order = lax.broadcasted_iota(jnp.int32, (SLOTS, 128), 0) + first_ref[0]
    order_square = order.astype(F32) * order.astype(F32)
    cosine = [jnp.broadcast_to(table_ref[0:1, 128 * h : 128 * h + 128], (SLOTS, 128)) for h in range(2)]
    diagonal = [table_ref[8 : 8 + SLOTS, 128 * h : 128 * h + 128] for h in range(2)]
    uni[0, 0:SLOTS, :] = jnp.zeros((SLOTS, 128), F32)
    empty = uni[0, 0:SLOTS, :]

    def advance(degree, carry):
        older, newer, down = carry
        value = jnp.full((8, 128), degree, jnp.int32).astype(F32)
        square = value * value
        inverse = 1.0 / (4.0 * square - 1.0)
        square = jnp.concatenate([square] * (SLOTS // 8))
        inverse = jnp.concatenate([inverse] * (SLOTS // 8))
        ratio = jnp.maximum((square - order_square) * inverse, 1e-30)
        up = lax.rsqrt(ratio)
        hit = order == degree
        made = []
        for h in range(2):
            row = jnp.where(hit, diagonal[h], up * (cosine[h] * newer[h] - down * older[h]))
            leg[h, pl.ds(degree, SLOTS, stride=LEG_PITCH), :] = row
            made.append(row)
        return newer, tuple(made), ratio * up

    def advance_some(turn, carry):
        for u in range(LEG_UNROLL):
            carry = advance(turn * LEG_UNROLL + u, carry)
        return carry

    lax.fori_loop(0, -(-degree_count // LEG_UNROLL), advance_some, ((empty, empty), (empty, empty), empty))
    fetch.wait()
    factor = math.sqrt(3.0) * math.sqrt(4.0 * math.pi) / degree_count * 2.0 ** (-30)

    def sum_degrees(m):
        spectral = (coef[:, m, :, :].astype(F32) * factor).reshape(pairs, degree_count).astype(BF16)
        for h in range(2):
            legendre = leg[h, pl.ds(m * LEG_PITCH, degree_count), :].astype(BF16)
            fourier = jnp.dot(spectral, legendre, preferred_element_type=F32)
            uni[h, pl.ds(m, pairs, stride=UNI_PITCH), :] = fourier

    def sum_two(turn, carry):
        sum_degrees(2 * turn)
        sum_degrees(2 * turn + 1)
        return carry

    lax.fori_loop(0, order_local // 2, sum_two, 0)
    blank = jnp.zeros((pairs, 128), F32)
    for h in range(2):
        for m in range(order_local, SLOTS):
            uni[h, pl.ds(m, pairs, stride=UNI_PITCH), :] = blank
    lane_group = lax.broadcasted_iota(jnp.int32, (2 * SLOTS, 128), 1) // 32

    def regroup(q, carry):
        for h in range(2):
            parts = [
                jnp.concatenate([uni[h, pl.ds((8 * q + 2 * i + p) * UNI_PITCH, SLOTS), :] for p in range(2)])
                for i in range(4)
            ]
            for group in range(4):
                joined = None
                for i in range(4):
                    turn = (i - group) % 4
                    moved = parts[i] if turn == 0 else pltpu.roll(parts[i], 32 * turn, 1)
                    joined = moved if joined is None else jnp.where(lane_group == i, moved, joined)
                joined = joined.astype(BF16)
                for j in range(3):
                    t = 3 * q + j
                    row = pl.multiple_of(32 * (t % 4), 32)
                    out_ref[4 * h + group, relative_part(t // 4, me), pl.ds(row, 32), :] = joined[32 * j : 32 * j + 32]
        return carry

    lax.fori_loop(0, channels // 4, regroup, 0)
    for s in range(8):
        out_ref[s, relative_part(15, me), 96:128, :] = jnp.zeros((32, 128), BF16)
    stores = [
        pltpu.make_async_copy(out_ref.at[:, pl.ds(8 * i, 8)], target, sems.at[1 + i])
        for i, target in ((1, away_hbm), (0, keep_hbm))
    ]
    for store in stores:
        store.start()
    for store in stores:
        store.wait()


def summed(parts):
    return functools.reduce(lambda a, b: a + b, [part.astype(F32) for part in parts])


def perturb_kernel(groups, scale_ref, me_ref, basis_ref, weather_ref, *refs):
    row_refs, mean_refs, out_ref, centred = refs[:2], refs[2:10], refs[10], refs[11]
    step = pl.program_id(0)
    me = me_ref[1]

    @pl.when(step == 0)
    def _():
        for k, mean_ref in enumerate(mean_refs):
            for dx in range(2):
                for s in range(8):
                    value = row_refs[k // 4][s, 2 * (k % 4) + dx].astype(F32) - mean_ref[s, dx].astype(F32)
                    centred[s, 2 * k + dx] = value.astype(BF16)

    columns = []
    for g in range(groups):
        pieces = []
        for s in range(8):
            for j in range(3):
                t = 3 * (step * groups + g) + j
                part = relative_part(t // 4, me)
                pieces.append(centred[s, part, pl.ds(pl.multiple_of(32 * (t % 4), 32), 32), :])
        columns.append(jnp.concatenate(pieces, axis=0))
    noise = lax.dot_general(
        jnp.concatenate(columns, axis=1), basis_ref[...], (((0,), (0,)), ((), ())), preferred_element_type=F32
    )
    for c in range(4 * groups):
        scale = scale_ref[step * 4 * groups + c]
        out_ref[c] = (weather_ref[c].astype(F32) + scale * noise[32 * c : 32 * c + 32]).astype(BF16)


def legendre_start(first_order, colatitude):
    orders = first_order + jnp.arange(SLOTS, dtype=jnp.int32)
    steps = jnp.arange(1, 384, dtype=jnp.int32)
    terms = 0.5 * jnp.log((2.0 * steps.astype(F32) + 1.0) / (2.0 * steps.astype(F32)))
    logs = jnp.sum(jnp.where(steps[None, :] <= orders[:, None], terms[None, :], 0.0), axis=1)
    diagonal = jnp.exp(
        logs[:, None]
        - 0.5 * math.log(4.0 * math.pi)
        + orders.astype(F32)[:, None] * jnp.log(jnp.sin(colatitude))[None, :]
    )
    cosine = jnp.broadcast_to(jnp.cos(colatitude)[None, :], (8, colatitude.shape[0]))
    return jnp.concatenate([cosine, diagonal])


def fourier_basis(bands, order_local, lon_count):
    slots = jnp.arange(SLOTS, dtype=jnp.int32)
    orders = order_local * jnp.arange(bands, dtype=jnp.int32)[:, None] + slots[None, :]
    columns = jnp.arange(lon_count, dtype=jnp.int32)
    phases = orders[:, :, None] * columns % lon_count
    angles = 2.0 * math.pi / lon_count * phases.astype(F32)
    weights = jnp.where(orders == 0, 1.0, math.sqrt(2.0))
    weights = jnp.where(slots[None, :] < order_local, weights, 0.0).astype(F32)[:, :, None]
    both = jnp.stack([weights * jnp.cos(angles), weights * jnp.sin(angles)], axis=1)
    return both.astype(BF16).reshape(bands * 2 * SLOTS, lon_count)


def local(weather, coefficients, channel_scale):
    members = lax.axis_size("member")
    bands = lax.axis_size("space")
    _, channels, rows_local, lon_count = weather.shape
    order_local, degree_count = coefficients.shape[3:]
    lat_count = rows_local * bands
    first_order = lax.axis_index("space") * order_local
    row_first = (lon_count // 2 + 1 - lat_count) // 2
    colatitude = math.pi * (row_first + jnp.arange(lat_count, dtype=jnp.int32)).astype(F32) / (lon_count // 2)
    vmem = pl.BlockSpec(memory_space=pltpu.VMEM)
    smem = pl.BlockSpec(memory_space=pltpu.SMEM)
    params = pltpu.CompilerParams(vmem_limit_bytes=VMEM)
    me = lax.axis_index("member")
    place = jnp.stack([first_order, me])
    ring = range(members)

    def to_core(x):
        return lax.ppermute(x, "member", [(e, e ^ 1) for e in ring])

    def to_chip(x):
        return lax.ppermute(x, "member", [(e, e ^ 2) for e in ring])

    def along_z(x, steps):
        return lax.ppermute(x, "member", [(e, (e + 4 * steps) % members) for e in ring])

    coef = jnp.transpose(coefficients[0], (0, 2, 1, 3))
    keep, away = pl.pallas_call(
        synthesis_kernel,
        in_specs=[smem, vmem, pl.BlockSpec(memory_space=pl.ANY)],
        out_specs=[pl.BlockSpec(memory_space=pl.ANY)] * 2,
        out_shape=[jax.ShapeDtypeStruct((bands, members // 2, 128, 128), BF16)] * 2,
        scratch_shapes=[
            pltpu.VMEM((channels, order_local, 2, degree_count), jnp.int32),
            pltpu.VMEM((2, SLOTS * LEG_PITCH + 8, 128), F32),
            pltpu.VMEM((2, 2 * channels * UNI_PITCH, 128), F32),
            pltpu.VMEM((bands, members, 128, 128), BF16),
            pltpu.SemaphoreType.DMA((3,)),
        ],
        compiler_params=params,
        name="synthesis",
    )(place, legendre_start(first_order, colatitude), coef)

    first_rows = lax.all_to_all(keep, "space", split_axis=0, concat_axis=0, tiled=True)
    got = to_core(away)
    sums = [summed([x[:, 2 * d : 2 * d + 2] for x in (keep, got)]).astype(BF16) for d in range(4)]
    arrived = [along_z(sums[d], d) for d in (2, 1, 3)]
    basis, sums[0] = lax.optimization_barrier((fourier_basis(bands, order_local, lon_count), sums[0]))
    column = summed([sums[0], *arrived]).astype(BF16)
    given = to_chip(column)[:, ::-1]
    mean = (summed([column, given]) * (1.0 / members)).astype(BF16)
    mean, first_rows = lax.optimization_barrier((mean, first_rows))
    mean = lax.all_to_all(mean, "space", split_axis=0, concat_axis=0, tiled=True)
    mean, away = lax.optimization_barrier((mean, away))
    last_rows = lax.all_to_all(away, "space", split_axis=0, concat_axis=0, tiled=True)
    tower = [mean] + [along_z(mean, 4 - d) for d in (1, 2, 3)]
    means = tower + [to_core(x) for x in tower]

    groups = 7
    band = pl.BlockSpec((4 * groups, rows_local, lon_count), lambda i: (i, 0, 0))
    perturbed = pl.pallas_call(
        functools.partial(perturb_kernel, groups),
        grid=(channels // (4 * groups),),
        in_specs=[
            smem,
            smem,
            pl.BlockSpec(basis.shape, lambda i: (0, 0)),
            band,
        ]
        + [pl.BlockSpec(keep.shape, lambda i: (0, 0, 0, 0))] * 2
        + [pl.BlockSpec(mean.shape, lambda i: (0, 0, 0, 0))] * 8,
        out_specs=band,
        out_shape=jax.ShapeDtypeStruct(weather.shape[1:], BF16),
        scratch_shapes=[pltpu.VMEM((bands, members, 128, 128), BF16)],
        compiler_params=params,
        name="perturb",
    )(channel_scale, place, basis, weather[0], first_rows, last_rows, *means)
    return perturbed[None]


def solution(mesh):
    return jax.shard_map(
        local,
        mesh=mesh,
        in_specs=(P("member", None, "space", None), P("member", None, None, "space", None), P()),
        out_specs=P("member", None, "space", None),
        check_vma=False,
    )
```

```python
import functools
import math

import jax
import jax.numpy as jnp
from jax import lax
from jax.experimental import pallas as pl
from jax.experimental.pallas import tpu as pltpu
from jax.sharding import PartitionSpec as P

F32 = jnp.float32
BF16 = jnp.bfloat16
SLOTS = 48
LEG_PITCH = 369
UNI_PITCH = 49
LEG_UNROLL = 16
VMEM = 60 * 2**20


def relative_part(part, me):
    return ((part ^ me) & 1) * 8 + ((part // 4 - me // 4) & 3) * 2 + (((part ^ me) // 2) & 1)


def synthesis_kernel(first_ref, table_ref, coef_hbm, keep_hbm, away_hbm, coef, leg, uni, out_ref, sems):
    channels, order_local, _, degree_count = coef.shape
    pairs = 2 * channels
    fetch = pltpu.make_async_copy(coef_hbm, coef, sems.at[0])
    fetch.start()
    me = first_ref[1]
    order = lax.broadcasted_iota(jnp.int32, (SLOTS, 128), 0) + first_ref[0]
    order_square = order.astype(F32) * order.astype(F32)
    cosine = [jnp.broadcast_to(table_ref[0:1, 128 * h : 128 * h + 128], (SLOTS, 128)) for h in range(2)]
    diagonal = [table_ref[8 : 8 + SLOTS, 128 * h : 128 * h + 128] for h in range(2)]
    uni[0, 0:SLOTS, :] = jnp.zeros((SLOTS, 128), F32)
    empty = uni[0, 0:SLOTS, :]

    def advance(degree, carry):
        older, newer, down = carry
        value = jnp.full((8, 128), degree, jnp.int32).astype(F32)
        square = value * value
        inverse = 1.0 / (4.0 * square - 1.0)
        square = jnp.concatenate([square] * (SLOTS // 8))
        inverse = jnp.concatenate([inverse] * (SLOTS // 8))
        ratio = jnp.maximum((square - order_square) * inverse, 1e-30)
        up = lax.rsqrt(ratio)
        hit = order == degree
        made = []
        for h in range(2):
            row = jnp.where(hit, diagonal[h], up * (cosine[h] * newer[h] - down * older[h]))
            leg[h, pl.ds(degree, SLOTS, stride=LEG_PITCH), :] = row
            made.append(row)
        return newer, tuple(made), ratio * up

    def advance_some(turn, carry):
        for u in range(LEG_UNROLL):
            carry = advance(turn * LEG_UNROLL + u, carry)
        return carry

    lax.fori_loop(0, -(-degree_count // LEG_UNROLL), advance_some, ((empty, empty), (empty, empty), empty))
    fetch.wait()
    factor = math.sqrt(3.0) * math.sqrt(4.0 * math.pi) / degree_count * 2.0 ** (-30)

    def sum_degrees(m):
        spectral = (coef[:, m, :, :].astype(F32) * factor).reshape(pairs, degree_count).astype(BF16)
        halves = [leg[h, pl.ds(m * LEG_PITCH, degree_count), :].astype(BF16) for h in range(2)]
        fourier = jnp.dot(spectral, jnp.concatenate(halves, axis=1), preferred_element_type=F32)
        for h in range(2):
            uni[h, pl.ds(m, pairs, stride=UNI_PITCH), :] = fourier[:, 128 * h : 128 * h + 128]

    def sum_two(turn, carry):
        sum_degrees(2 * turn)
        sum_degrees(2 * turn + 1)
        return carry

    lax.fori_loop(0, order_local // 2, sum_two, 0)
    blank = jnp.zeros((pairs, 128), F32)
    for h in range(2):
        for m in range(order_local, SLOTS):
            uni[h, pl.ds(m, pairs, stride=UNI_PITCH), :] = blank
    lane_group = lax.broadcasted_iota(jnp.int32, (2 * SLOTS, 128), 1) // 32

    def regroup(q, carry):
        for h in range(2):
            parts = [
                jnp.concatenate([uni[h, pl.ds((8 * q + 2 * i + p) * UNI_PITCH, SLOTS), :] for p in range(2)])
                for i in range(4)
            ]
            for group in range(4):
                joined = None
                for i in range(4):
                    turn = (i - group) % 4
                    moved = parts[i] if turn == 0 else pltpu.roll(parts[i], 32 * turn, 1)
                    joined = moved if joined is None else jnp.where(lane_group == i, moved, joined)
                joined = joined.astype(BF16)
                for j in range(3):
                    t = 3 * q + j
                    row = pl.multiple_of(32 * (t % 4), 32)
                    out_ref[4 * h + group, relative_part(t // 4, me), pl.ds(row, 32), :] = joined[32 * j : 32 * j + 32]
        return carry

    lax.fori_loop(0, channels // 4, regroup, 0, unroll=3)
    for s in range(8):
        out_ref[s, relative_part(15, me), 96:128, :] = jnp.zeros((32, 128), BF16)
    stores = [
        pltpu.make_async_copy(out_ref.at[:, pl.ds(8 * i, 8)], target, sems.at[1 + i])
        for i, target in ((1, away_hbm), (0, keep_hbm))
    ]
    for store in stores:
        store.start()
    for store in stores:
        store.wait()


def summed(parts):
    return functools.reduce(lambda a, b: a + b, [part.astype(F32) for part in parts])


def perturb_kernel(groups, scale_ref, me_ref, basis_ref, weather_ref, *refs):
    row_refs, mean_refs, out_ref, centred = refs[:2], refs[2:12], refs[12], refs[13]
    step = pl.program_id(0)
    me = me_ref[1]

    @pl.when(step == 0)
    def _():
        for half, row_ref in enumerate(row_refs):
            for i, (piece, dx) in enumerate(((0, 0), (0, 1), (1, 0), (1, 1), (2, 0), (3, 0), (4, 0), (4, 1))):
                for s in range(8):
                    value = row_ref[s, i].astype(F32) - mean_refs[5 * half + piece][s, dx].astype(F32)
                    centred[s, 8 * half + i] = value.astype(BF16)

    columns = []
    for g in range(groups):
        pieces = []
        for s in range(8):
            for j in range(3):
                t = 3 * (step * groups + g) + j
                part = relative_part(t // 4, me)
                pieces.append(centred[s, part, pl.ds(pl.multiple_of(32 * (t % 4), 32), 32), :])
        columns.append(jnp.concatenate(pieces, axis=0))
    noise = lax.dot_general(
        jnp.concatenate(columns, axis=1), basis_ref[...], (((0,), (0,)), ((), ())), preferred_element_type=F32
    )
    for c in range(4 * groups):
        scale = scale_ref[step * 4 * groups + c]
        out_ref[c] = (weather_ref[c].astype(F32) + scale * noise[32 * c : 32 * c + 32]).astype(BF16)


def legendre_start(first_order, colatitude):
    orders = first_order + jnp.arange(SLOTS, dtype=jnp.int32)
    steps = jnp.arange(1, 384, dtype=jnp.int32)
    terms = 0.5 * jnp.log((2.0 * steps.astype(F32) + 1.0) / (2.0 * steps.astype(F32)))
    logs = jnp.sum(jnp.where(steps[None, :] <= orders[:, None], terms[None, :], 0.0), axis=1)
    diagonal = jnp.exp(
        logs[:, None]
        - 0.5 * math.log(4.0 * math.pi)
        + orders.astype(F32)[:, None] * jnp.log(jnp.sin(colatitude))[None, :]
    )
    cosine = jnp.broadcast_to(jnp.cos(colatitude)[None, :], (8, colatitude.shape[0]))
    return jnp.concatenate([cosine, diagonal])


def fourier_basis(bands, order_local, lon_count):
    slots = jnp.arange(SLOTS, dtype=jnp.int32)
    orders = order_local * jnp.arange(bands, dtype=jnp.int32)[:, None] + slots[None, :]
    columns = jnp.arange(lon_count, dtype=jnp.int32)
    phases = orders[:, :, None] * columns % lon_count
    angles = 2.0 * math.pi / lon_count * phases.astype(F32)
    weights = jnp.where(orders == 0, 1.0, math.sqrt(2.0))
    weights = jnp.where(slots[None, :] < order_local, weights, 0.0).astype(F32)[:, :, None]
    both = jnp.stack([weights * jnp.cos(angles), weights * jnp.sin(angles)], axis=1)
    return both.astype(BF16).reshape(bands * 2 * SLOTS, lon_count)


def local(weather, coefficients, channel_scale):
    members = lax.axis_size("member")
    bands = lax.axis_size("space")
    _, channels, rows_local, lon_count = weather.shape
    order_local, degree_count = coefficients.shape[3:]
    lat_count = rows_local * bands
    first_order = lax.axis_index("space") * order_local
    row_first = (lon_count // 2 + 1 - lat_count) // 2
    colatitude = math.pi * (row_first + jnp.arange(lat_count, dtype=jnp.int32)).astype(F32) / (lon_count // 2)
    vmem = pl.BlockSpec(memory_space=pltpu.VMEM)
    smem = pl.BlockSpec(memory_space=pltpu.SMEM)
    params = pltpu.CompilerParams(vmem_limit_bytes=VMEM)
    me = lax.axis_index("member")
    place = jnp.stack([first_order, me])
    ring = range(members)

    def to_core(x):
        return lax.ppermute(x, "member", [(e, e ^ 1) for e in ring])

    def to_chip(x):
        return lax.ppermute(x, "member", [(e, e ^ 2) for e in ring])

    def along_z(x, steps):
        return lax.ppermute(x, "member", [(e, (e + 4 * steps) % members) for e in ring])

    coef = jnp.transpose(coefficients[0], (0, 2, 1, 3))
    keep, away = pl.pallas_call(
        synthesis_kernel,
        in_specs=[smem, vmem, pl.BlockSpec(memory_space=pl.ANY)],
        out_specs=[pl.BlockSpec(memory_space=pl.ANY)] * 2,
        out_shape=[jax.ShapeDtypeStruct((bands, members // 2, 128, 128), BF16)] * 2,
        scratch_shapes=[
            pltpu.VMEM((channels, order_local, 2, degree_count), jnp.int32),
            pltpu.VMEM((2, SLOTS * LEG_PITCH + 8, 128), F32),
            pltpu.VMEM((2, 2 * channels * UNI_PITCH, 128), F32),
            pltpu.VMEM((bands, members, 128, 128), BF16),
            pltpu.SemaphoreType.DMA((3,)),
        ],
        compiler_params=params,
        name="synthesis",
    )(place, legendre_start(first_order, colatitude), coef)

    first_rows = lax.all_to_all(keep, "space", split_axis=0, concat_axis=0, tiled=True)
    got = to_core(away)
    sums = [summed([x[:, 2 * d : 2 * d + 2] for x in (keep, got)]).astype(BF16) for d in range(4)]
    far = sums[2]
    up, down = along_z(far[:, :1], 1), along_z(far[:, 1:], 3)
    up = jnp.concatenate([summed([sums[1][:, :1], up]).astype(BF16), sums[1][:, 1:]], axis=1)
    down = jnp.concatenate([sums[3][:, :1], summed([sums[3][:, 1:], down]).astype(BF16)], axis=1)
    arrived = [along_z(up, 1), along_z(down, 3)]
    basis, own = lax.optimization_barrier((fourier_basis(bands, order_local, lon_count), sums[0]))
    column = summed([own, *arrived]).astype(BF16)
    given = to_chip(column)[:, ::-1]
    mean = (summed([column, given]) * (1.0 / members)).astype(BF16)
    mean, first_rows = lax.optimization_barrier((mean, first_rows))
    mean = lax.all_to_all(mean, "space", split_axis=0, concat_axis=0, tiled=True)
    mean, away = lax.optimization_barrier((mean, away))
    last_rows = lax.all_to_all(away, "space", split_axis=0, concat_axis=0, tiled=True)
    below, above = along_z(mean, 1), along_z(mean, 3)
    far = [along_z(below[:, :1], 1), along_z(above[:, 1:], 3)]
    tower = [mean, above, *far, below]
    means = tower + [to_core(x) for x in tower]

    groups = 7
    once = pl.Buffered(1)
    band = pl.BlockSpec((4 * groups, rows_local, lon_count), lambda i: (i, 0, 0))
    perturbed = pl.pallas_call(
        functools.partial(perturb_kernel, groups),
        grid=(channels // (4 * groups),),
        in_specs=[
            smem,
            smem,
            pl.BlockSpec(basis.shape, lambda i: (0, 0), pipeline_mode=once),
            band,
        ]
        + [pl.BlockSpec(keep.shape, lambda i: (0, 0, 0, 0), pipeline_mode=once)] * 2
        + [pl.BlockSpec(x.shape, lambda i: (0, 0, 0, 0), pipeline_mode=once) for x in means],
        out_specs=band,
        out_shape=jax.ShapeDtypeStruct(weather.shape[1:], BF16),
        scratch_shapes=[pltpu.VMEM((bands, members, 128, 128), BF16)],
        compiler_params=pltpu.CompilerParams(vmem_limit_bytes=60 * 2**20),
        name="perturb",
    )(channel_scale, place, basis, weather[0], first_rows, last_rows, *means)
    return perturbed[None]


def solution(mesh):
    return jax.shard_map(
        local,
        mesh=mesh,
        in_specs=(P("member", None, "space", None), P("member", None, None, "space", None), P()),
        out_specs=P("member", None, "space", None),
        check_vma=False,
    )
```

```python
import functools
import math

import jax
import jax.numpy as jnp
from jax import lax
from jax.experimental import pallas as pl
from jax.experimental.pallas import tpu as pltpu
from jax.sharding import PartitionSpec as P


F32 = jnp.float32
BF16 = jnp.bfloat16
SLOTS = 48
LEG_PITCH = 369
UNI_PITCH = 49
LEG_UNROLL = 16
EARLY = 10
VMEM = 60 * 2**20


def relative_part(part, me):
    return ((part ^ me) & 1) * 8 + ((part // 4 - me // 4) & 3) * 2 + (((part ^ me) // 2) & 1)


def synthesis_kernel(first_ref, table_ref, coef_hbm, first_hbm, rest_hbm, away_hbm, coef, leg, uni, out_ref, sems):
    channels, order_local, _, degree_count = coef.shape
    pairs = 2 * channels
    fetch = pltpu.make_async_copy(coef_hbm, coef, sems.at[0])
    fetch.start()
    me = first_ref[1]
    order = lax.broadcasted_iota(jnp.int32, (SLOTS, 128), 0) + first_ref[0]
    order_square = order.astype(F32) * order.astype(F32)
    cosine = [jnp.broadcast_to(table_ref[0:1, 128 * h : 128 * h + 128], (SLOTS, 128)) for h in range(2)]
    diagonal = [table_ref[8 : 8 + SLOTS, 128 * h : 128 * h + 128] for h in range(2)]
    uni[0, 0:SLOTS, :] = jnp.zeros((SLOTS, 128), F32)
    empty = uni[0, 0:SLOTS, :]

    def advance(degree, carry):
        older, newer, down = carry
        value = jnp.full((8, 128), degree, jnp.int32).astype(F32)
        square = value * value
        inverse = 1.0 / (4.0 * square - 1.0)
        square = jnp.concatenate([square] * (SLOTS // 8))
        inverse = jnp.concatenate([inverse] * (SLOTS // 8))
        ratio = jnp.maximum((square - order_square) * inverse, 1e-30)
        up = lax.rsqrt(ratio)
        hit = order == degree
        made = []
        for h in range(2):
            row = jnp.where(hit, diagonal[h], up * (cosine[h] * newer[h] - down * older[h]))
            leg[h, pl.ds(degree, SLOTS, stride=LEG_PITCH), :] = row
            made.append(row)
        return newer, tuple(made), ratio * up

    def advance_some(turn, carry):
        for u in range(LEG_UNROLL):
            carry = advance(turn * LEG_UNROLL + u, carry)
        return carry

    lax.fori_loop(0, -(-degree_count // LEG_UNROLL), advance_some, ((empty, empty), (empty, empty), empty))
    fetch.wait()
    factor = math.sqrt(3.0) * math.sqrt(4.0 * math.pi) / degree_count * 2.0 ** (-30)

    def sum_degrees(m):
        spectral = (coef[:, m, :, :].astype(F32) * factor).reshape(pairs, degree_count).astype(BF16)
        halves = [leg[h, pl.ds(m * LEG_PITCH, degree_count), :].astype(BF16) for h in range(2)]
        fourier = jnp.dot(spectral, jnp.concatenate(halves, axis=1), preferred_element_type=F32)
        for h in range(2):
            uni[h, pl.ds(m, pairs, stride=UNI_PITCH), :] = fourier[:, 128 * h : 128 * h + 128]

    def sum_two(turn, carry):
        sum_degrees(2 * turn)
        sum_degrees(2 * turn + 1)
        return carry

    lax.fori_loop(0, order_local // 2, sum_two, 0)
    blank = jnp.zeros((pairs, 128), F32)
    for h in range(2):
        for m in range(order_local, SLOTS):
            uni[h, pl.ds(m, pairs, stride=UNI_PITCH), :] = blank
    lane_group = lax.broadcasted_iota(jnp.int32, (2 * SLOTS, 128), 1) // 32

    def regroup(q, carry):
        for h in range(2):
            parts = [
                jnp.concatenate([uni[h, pl.ds((8 * q + 2 * i + p) * UNI_PITCH, SLOTS), :] for p in range(2)])
                for i in range(4)
            ]
            for group in range(4):
                joined = None
                for i in range(4):
                    turn = (i - group) % 4
                    moved = parts[i] if turn == 0 else pltpu.roll(parts[i], 32 * turn, 1)
                    joined = moved if joined is None else jnp.where(lane_group == i, moved, joined)
                joined = joined.astype(BF16)
                for j in range(3):
                    t = 3 * q + j
                    row = pl.multiple_of(32 * (t % 4), 32)
                    out_ref[4 * h + group, relative_part(t // 4, me), pl.ds(row, 32), :] = joined[32 * j : 32 * j + 32]
        return carry

    def store(part, act):
        place = relative_part(part, me)

        @pl.when(place < EARLY)
        def _():
            act(pltpu.make_async_copy(out_ref.at[:, place], first_hbm.at[:, place], sems.at[1 + part]))

        @pl.when(place >= EARLY)
        def _():
            act(pltpu.make_async_copy(out_ref.at[:, place], rest_hbm.at[:, place - EARLY], sems.at[1 + part]))

        @pl.when(place >= 8)
        def _():
            act(pltpu.make_async_copy(out_ref.at[:, place], away_hbm.at[:, place - 8], sems.at[17 + part]))

    done = 0
    for first, last in ((0, 6), (6, 12), (12, 18), (18, channels // 4)):
        lax.fori_loop(first, last, regroup, 0, unroll=3)
        if last == channels // 4:
            for s in range(8):
                out_ref[s, relative_part(15, me), 96:128, :] = jnp.zeros((32, 128), BF16)
        whole = 16 if last == channels // 4 else 3 * last // 4
        for part in range(done, whole):
            store(part, lambda copy: copy.start())
        done = whole
    for part in range(16):
        store(part, lambda copy: copy.wait())


def summed(parts):
    return functools.reduce(lambda a, b: a + b, [part.astype(F32) for part in parts])


def perturb_kernel(groups, scale_ref, me_ref, basis_ref, weather_ref, *refs):
    row_refs, mean_refs, out_ref, centred = refs[:2], refs[2:12], refs[12], refs[13]
    step = pl.program_id(0)
    me = me_ref[1]

    @pl.when(step == 0)
    def _():
        places = ((0, 0), (0, 1), (1, 0), (1, 1), (2, 0), (3, 0), (4, 0), (4, 1))
        for i in range(16):
            piece, dx = places[i % 8]
            for s in range(8):
                row = row_refs[0][s, i] if i < EARLY else row_refs[1][s, i - EARLY]
                value = row.astype(F32) - mean_refs[5 * (i // 8) + piece][s, dx].astype(F32)
                centred[s, i] = value.astype(BF16)

    columns = []
    for g in range(groups):
        pieces = []
        for s in range(8):
            for j in range(3):
                t = 3 * (step * groups + g) + j
                part = relative_part(t // 4, me)
                pieces.append(centred[s, part, pl.ds(pl.multiple_of(32 * (t % 4), 32), 32), :])
        columns.append(jnp.concatenate(pieces, axis=0))
    noise = lax.dot_general(
        jnp.concatenate(columns, axis=1), basis_ref[...], (((0,), (0,)), ((), ())), preferred_element_type=F32
    )
    for c in range(4 * groups):
        scale = scale_ref[step * 4 * groups + c]
        out_ref[c] = (weather_ref[c].astype(F32) + scale * noise[32 * c : 32 * c + 32]).astype(BF16)


def legendre_start(first_order, colatitude):
    orders = first_order + jnp.arange(SLOTS, dtype=jnp.int32)
    steps = jnp.arange(1, 384, dtype=jnp.int32)
    terms = 0.5 * jnp.log((2.0 * steps.astype(F32) + 1.0) / (2.0 * steps.astype(F32)))
    logs = jnp.sum(jnp.where(steps[None, :] <= orders[:, None], terms[None, :], 0.0), axis=1)
    diagonal = jnp.exp(
        logs[:, None]
        - 0.5 * math.log(4.0 * math.pi)
        + orders.astype(F32)[:, None] * jnp.log(jnp.sin(colatitude))[None, :]
    )
    cosine = jnp.broadcast_to(jnp.cos(colatitude)[None, :], (8, colatitude.shape[0]))
    return jnp.concatenate([cosine, diagonal])


def fourier_basis(bands, order_local, lon_count):
    slots = jnp.arange(SLOTS, dtype=jnp.int32)
    orders = order_local * jnp.arange(bands, dtype=jnp.int32)[:, None] + slots[None, :]
    columns = jnp.arange(lon_count, dtype=jnp.int32)
    phases = orders[:, :, None] * columns % lon_count
    angles = 2.0 * math.pi / lon_count * phases.astype(F32)
    weights = jnp.where(orders == 0, 1.0, math.sqrt(2.0))
    weights = jnp.where(slots[None, :] < order_local, weights, 0.0).astype(F32)[:, :, None]
    both = jnp.stack([weights * jnp.cos(angles), weights * jnp.sin(angles)], axis=1)
    return both.astype(BF16).reshape(bands * 2 * SLOTS, lon_count)


def local(weather, coefficients, channel_scale):
    members = lax.axis_size("member")
    bands = lax.axis_size("space")
    _, channels, rows_local, lon_count = weather.shape
    order_local, degree_count = coefficients.shape[3:]
    lat_count = rows_local * bands
    first_order = lax.axis_index("space") * order_local
    row_first = (lon_count // 2 + 1 - lat_count) // 2
    colatitude = math.pi * (row_first + jnp.arange(lat_count, dtype=jnp.int32)).astype(F32) / (lon_count // 2)
    vmem = pl.BlockSpec(memory_space=pltpu.VMEM)
    smem = pl.BlockSpec(memory_space=pltpu.SMEM)
    params = pltpu.CompilerParams(vmem_limit_bytes=VMEM)
    me = lax.axis_index("member")
    place = jnp.stack([first_order, me])
    ring = range(members)

    def to_core(x):
        return lax.ppermute(x, "member", [(e, e ^ 1) for e in ring])

    def to_chip(x):
        return lax.ppermute(x, "member", [(e, e ^ 2) for e in ring])

    def along_z(x, steps):
        return lax.ppermute(x, "member", [(e, (e + 4 * steps) % members) for e in ring])

    coef = jnp.transpose(coefficients[0], (0, 2, 1, 3))
    first, rest, away = pl.pallas_call(
        synthesis_kernel,
        in_specs=[smem, vmem, pl.BlockSpec(memory_space=pl.ANY)],
        out_specs=[pl.BlockSpec(memory_space=pl.ANY)] * 3,
        out_shape=[jax.ShapeDtypeStruct((bands, n, 128, 128), BF16) for n in (EARLY, members - EARLY, 8)],
        scratch_shapes=[
            pltpu.VMEM((channels, order_local, 2, degree_count), jnp.int32),
            pltpu.VMEM((2, SLOTS * LEG_PITCH + 8, 128), F32),
            pltpu.VMEM((2, 2 * channels * UNI_PITCH, 128), F32),
            pltpu.VMEM((bands, members, 128, 128), BF16),
            pltpu.SemaphoreType.DMA((33,)),
        ],
        compiler_params=params,
        name="synthesis",
    )(place, legendre_start(first_order, colatitude), coef)

    first_rows = lax.all_to_all(first, "space", split_axis=0, concat_axis=0, tiled=True)
    got = to_core(away)
    sums = [summed([x[:, 2 * d : 2 * d + 2] for x in (first, got)]).astype(BF16) for d in range(4)]
    far = sums[2]
    up = along_z(far[:, :1], 1)
    down = along_z(far[:, 1:], 3)
    up = jnp.concatenate([summed([sums[1][:, :1], up]).astype(BF16), sums[1][:, 1:]], axis=1)
    down = jnp.concatenate([sums[3][:, :1], summed([sums[3][:, 1:], down]).astype(BF16)], axis=1)
    arrived = [along_z(up, 1), along_z(down, 3)]
    basis, own = lax.optimization_barrier((fourier_basis(bands, order_local, lon_count), sums[0]))
    column = summed([own, *arrived]).astype(BF16)
    given = to_chip(column)[:, ::-1]
    mean = (summed([column, given]) * (1.0 / members)).astype(BF16)
    mean, first_rows = lax.optimization_barrier((mean, first_rows))
    mean = lax.all_to_all(mean, "space", split_axis=0, concat_axis=0, tiled=True)
    mean, rest = lax.optimization_barrier((mean, rest))
    last_rows = lax.all_to_all(rest, "space", split_axis=0, concat_axis=0, tiled=True)
    below = along_z(mean, 1)
    above = along_z(mean, 3)
    far_up = along_z(below[:, :1], 1)
    far_down = along_z(above[:, 1:], 3)
    other = [to_core(mean)]
    other.append(to_core(above))
    other += [to_core(far_up), to_core(far_down)]
    other.append(to_core(below))
    means = [mean, above, far_up, far_down, below, *other]

    groups = 7
    once = pl.Buffered(1)
    band = pl.BlockSpec((4 * groups, rows_local, lon_count), lambda i: (i, 0, 0))
    perturbed = pl.pallas_call(
        functools.partial(perturb_kernel, groups),
        grid=(channels // (4 * groups),),
        in_specs=[
            smem,
            smem,
            pl.BlockSpec(basis.shape, lambda i: (0, 0), pipeline_mode=once),
            band,
        ]
        + [pl.BlockSpec(x.shape, lambda i: (0, 0, 0, 0), pipeline_mode=once) for x in (first, rest, *means)],
        out_specs=band,
        out_shape=jax.ShapeDtypeStruct(weather.shape[1:], BF16),
        scratch_shapes=[pltpu.VMEM((bands, members, 128, 128), BF16)],
        compiler_params=pltpu.CompilerParams(vmem_limit_bytes=60 * 2**20),
        name="perturb",
    )(channel_scale, place, basis, weather[0], first_rows, last_rows, *means)
    return perturbed[None]


def solution(mesh):
    return jax.shard_map(
        local,
        mesh=mesh,
        in_specs=(P("member", None, "space", None), P("member", None, None, "space", None), P()),
        out_specs=P("member", None, "space", None),
        check_vma=False,
    )
```

```python
import functools
import math

import jax
import jax.numpy as jnp
from jax import lax
from jax.experimental import pallas as pl
from jax.experimental.pallas import tpu as pltpu
from jax.sharding import PartitionSpec as P


F32 = jnp.float32
BF16 = jnp.bfloat16
SLOTS = 48
LEG_PITCH = 369
UNI_PITCH = 49
LEG_UNROLL = 16
EARLY = 10
VMEM = 60 * 2**20


def relative_part(part, me):
    return ((part ^ me) & 1) * 8 + ((part // 4 - me // 4) & 3) * 2 + (((part ^ me) // 2) & 1)


def synthesis_kernel(first_ref, table_ref, coef_hbm, first_hbm, rest_hbm, away_hbm, coef, leg, uni, out_ref, sems):
    channels, order_local, _, degree_count = coef.shape
    pairs = 2 * channels
    fetch = pltpu.make_async_copy(coef_hbm, coef, sems.at[0])
    fetch.start()
    me = first_ref[1]
    order = lax.broadcasted_iota(jnp.int32, (SLOTS, 128), 0) + first_ref[0]
    order_square = order.astype(F32) * order.astype(F32)
    cosine = [jnp.broadcast_to(table_ref[0:1, 128 * h : 128 * h + 128], (SLOTS, 128)) for h in range(2)]
    diagonal = [table_ref[8 : 8 + SLOTS, 128 * h : 128 * h + 128] for h in range(2)]
    uni[0, 0:SLOTS, :] = jnp.zeros((SLOTS, 128), F32)
    empty = uni[0, 0:SLOTS, :]

    def advance(degree, carry):
        older, newer, down = carry
        value = jnp.full((8, 128), degree, jnp.int32).astype(F32)
        square = value * value
        inverse = 1.0 / (4.0 * square - 1.0)
        square = jnp.concatenate([square] * (SLOTS // 8))
        inverse = jnp.concatenate([inverse] * (SLOTS // 8))
        ratio = jnp.maximum((square - order_square) * inverse, 1e-30)
        up = lax.rsqrt(ratio)
        hit = order == degree
        made = []
        for h in range(2):
            row = jnp.where(hit, diagonal[h], up * (cosine[h] * newer[h] - down * older[h]))
            leg[h, pl.ds(degree, SLOTS, stride=LEG_PITCH), :] = row
            made.append(row)
        return newer, tuple(made), ratio * up

    def advance_some(turn, carry):
        for u in range(LEG_UNROLL):
            carry = advance(turn * LEG_UNROLL + u, carry)
        return carry

    lax.fori_loop(0, -(-degree_count // LEG_UNROLL), advance_some, ((empty, empty), (empty, empty), empty))
    fetch.wait()
    factor = math.sqrt(3.0) * math.sqrt(4.0 * math.pi) / degree_count * 2.0 ** (-30)

    def sum_degrees(m):
        spectral = (coef[:, m, :, :].astype(F32) * factor).reshape(pairs, degree_count).astype(BF16)
        halves = [leg[h, pl.ds(m * LEG_PITCH, degree_count), :].astype(BF16) for h in range(2)]
        fourier = jnp.dot(spectral, jnp.concatenate(halves, axis=1), preferred_element_type=F32)
        for h in range(2):
            uni[h, pl.ds(m, pairs, stride=UNI_PITCH), :] = fourier[:, 128 * h : 128 * h + 128]

    def sum_four(turn, carry):
        for u in range(4):
            sum_degrees(4 * turn + u)
        return carry

    lax.fori_loop(0, order_local // 4, sum_four, 0)
    for m in range(order_local - order_local % 4, order_local):
        sum_degrees(m)
    blank = jnp.zeros((pairs, 128), F32)
    for h in range(2):
        for m in range(order_local, SLOTS):
            uni[h, pl.ds(m, pairs, stride=UNI_PITCH), :] = blank
    lane_group = lax.broadcasted_iota(jnp.int32, (2 * SLOTS, 128), 1) // 32

    def regroup(q, carry):
        for h in range(2):
            parts = [
                jnp.concatenate([uni[h, pl.ds((8 * q + 2 * i + p) * UNI_PITCH, SLOTS), :] for p in range(2)])
                for i in range(4)
            ]
            for group in range(4):
                joined = None
                for i in range(4):
                    turn = (i - group) % 4
                    moved = parts[i] if turn == 0 else pltpu.roll(parts[i], 32 * turn, 1)
                    joined = moved if joined is None else jnp.where(lane_group == i, moved, joined)
                joined = joined.astype(BF16)
                for j in range(3):
                    t = 3 * q + j
                    row = pl.multiple_of(32 * (t % 4), 32)
                    out_ref[4 * h + group, relative_part(t // 4, me), pl.ds(row, 32), :] = joined[32 * j : 32 * j + 32]
        return carry

    def store(part, act):
        place = relative_part(part, me)

        @pl.when(place < EARLY)
        def _():
            act(pltpu.make_async_copy(out_ref.at[:, place], first_hbm.at[:, place], sems.at[1 + part]))

        @pl.when(place >= EARLY)
        def _():
            act(pltpu.make_async_copy(out_ref.at[:, place], rest_hbm.at[:, place - EARLY], sems.at[1 + part]))

        @pl.when(place >= 8)
        def _():
            act(pltpu.make_async_copy(out_ref.at[:, place], away_hbm.at[:, place - 8], sems.at[17 + part]))

    done = 0
    for first, last in ((0, 6), (6, 12), (12, 18), (18, channels // 4)):
        lax.fori_loop(first, last, regroup, 0, unroll=3)
        if last == channels // 4:
            for s in range(8):
                out_ref[s, relative_part(15, me), 96:128, :] = jnp.zeros((32, 128), BF16)
        whole = 16 if last == channels // 4 else 3 * last // 4
        for part in range(done, whole):
            store(part, lambda copy: copy.start())
        done = whole
    for part in range(16):
        store(part, lambda copy: copy.wait())


def summed(parts):
    return functools.reduce(lambda a, b: a + b, [part.astype(F32) for part in parts])


def perturb_kernel(groups, scale_ref, me_ref, basis_ref, weather_ref, *refs):
    row_refs, mean_refs, out_ref, centred = refs[:2], refs[2:12], refs[12], refs[13]
    step = pl.program_id(0)
    me = me_ref[1]

    @pl.when(step == 0)
    def _():
        places = ((0, 0), (0, 1), (1, 0), (1, 1), (2, 0), (3, 0), (4, 0), (4, 1))
        for i in range(16):
            piece, dx = places[i % 8]
            for s in range(8):
                row = row_refs[0][s, i] if i < EARLY else row_refs[1][s, i - EARLY]
                value = row.astype(F32) - mean_refs[5 * (i // 8) + piece][s, dx].astype(F32)
                centred[s, i] = value.astype(BF16)

    columns = []
    for g in range(groups):
        pieces = []
        for s in range(8):
            for j in range(3):
                t = 3 * (step * groups + g) + j
                part = relative_part(t // 4, me)
                pieces.append(centred[s, part, pl.ds(pl.multiple_of(32 * (t % 4), 32), 32), :])
        columns.append(jnp.concatenate(pieces, axis=0))
    noise = lax.dot_general(
        jnp.concatenate(columns, axis=1), basis_ref[...], (((0,), (0,)), ((), ())), preferred_element_type=F32
    )
    for c in range(4 * groups):
        scale = scale_ref[step * 4 * groups + c]
        out_ref[c] = (weather_ref[c].astype(F32) + scale * noise[32 * c : 32 * c + 32]).astype(BF16)


def legendre_start(first_order, colatitude):
    orders = first_order + jnp.arange(SLOTS, dtype=jnp.int32)
    steps = jnp.arange(1, 384, dtype=jnp.int32)
    terms = 0.5 * jnp.log((2.0 * steps.astype(F32) + 1.0) / (2.0 * steps.astype(F32)))
    logs = jnp.sum(jnp.where(steps[None, :] <= orders[:, None], terms[None, :], 0.0), axis=1)
    diagonal = jnp.exp(
        logs[:, None]
        - 0.5 * math.log(4.0 * math.pi)
        + orders.astype(F32)[:, None] * jnp.log(jnp.sin(colatitude))[None, :]
    )
    cosine = jnp.broadcast_to(jnp.cos(colatitude)[None, :], (8, colatitude.shape[0]))
    return jnp.concatenate([cosine, diagonal])


def fourier_basis(bands, order_local, lon_count):
    slots = jnp.arange(SLOTS, dtype=jnp.int32)
    orders = order_local * jnp.arange(bands, dtype=jnp.int32)[:, None] + slots[None, :]
    columns = jnp.arange(lon_count, dtype=jnp.int32)
    phases = orders[:, :, None] * columns % lon_count
    angles = 2.0 * math.pi / lon_count * phases.astype(F32)
    weights = jnp.where(orders == 0, 1.0, math.sqrt(2.0))
    weights = jnp.where(slots[None, :] < order_local, weights, 0.0).astype(F32)[:, :, None]
    both = jnp.stack([weights * jnp.cos(angles), weights * jnp.sin(angles)], axis=1)
    return both.astype(BF16).reshape(bands * 2 * SLOTS, lon_count)


def local(weather, coefficients, channel_scale):
    members = lax.axis_size("member")
    bands = lax.axis_size("space")
    _, channels, rows_local, lon_count = weather.shape
    order_local, degree_count = coefficients.shape[3:]
    lat_count = rows_local * bands
    first_order = lax.axis_index("space") * order_local
    row_first = (lon_count // 2 + 1 - lat_count) // 2
    colatitude = math.pi * (row_first + jnp.arange(lat_count, dtype=jnp.int32)).astype(F32) / (lon_count // 2)
    vmem = pl.BlockSpec(memory_space=pltpu.VMEM)
    smem = pl.BlockSpec(memory_space=pltpu.SMEM)
    params = pltpu.CompilerParams(vmem_limit_bytes=VMEM)
    me = lax.axis_index("member")
    place = jnp.stack([first_order, me])
    ring = range(members)

    def to_core(x):
        return lax.ppermute(x, "member", [(e, e ^ 1) for e in ring])

    def to_chip(x):
        return lax.ppermute(x, "member", [(e, e ^ 2) for e in ring])

    def along_z(x, steps):
        return lax.ppermute(x, "member", [(e, (e + 4 * steps) % members) for e in ring])

    coef = jnp.transpose(coefficients[0], (0, 2, 1, 3))
    first, rest, away = pl.pallas_call(
        synthesis_kernel,
        in_specs=[smem, vmem, pl.BlockSpec(memory_space=pl.ANY)],
        out_specs=[pl.BlockSpec(memory_space=pl.ANY)] * 3,
        out_shape=[jax.ShapeDtypeStruct((bands, n, 128, 128), BF16) for n in (EARLY, members - EARLY, 8)],
        scratch_shapes=[
            pltpu.VMEM((channels, order_local, 2, degree_count), jnp.int32),
            pltpu.VMEM((2, SLOTS * LEG_PITCH + 8, 128), F32),
            pltpu.VMEM((2, 2 * channels * UNI_PITCH, 128), F32),
            pltpu.VMEM((bands, members, 128, 128), BF16),
            pltpu.SemaphoreType.DMA((33,)),
        ],
        compiler_params=params,
        name="synthesis",
    )(place, legendre_start(first_order, colatitude), coef)

    first_rows = lax.all_to_all(first, "space", split_axis=0, concat_axis=0, tiled=True)
    got = to_core(away)
    sums = [summed([x[:, 2 * d : 2 * d + 2] for x in (first, got)]).astype(BF16) for d in range(4)]
    far = sums[2]
    up = along_z(far[:, :1], 1)
    down = along_z(far[:, 1:], 3)
    up = jnp.concatenate([summed([sums[1][:, :1], up]).astype(BF16), sums[1][:, 1:]], axis=1)
    down = jnp.concatenate([sums[3][:, :1], summed([sums[3][:, 1:], down]).astype(BF16)], axis=1)
    arrived = [along_z(up, 1), along_z(down, 3)]
    basis, own = lax.optimization_barrier((fourier_basis(bands, order_local, lon_count), sums[0]))
    column = summed([own, *arrived]).astype(BF16)
    given = to_chip(column)[:, ::-1]
    mean = (summed([column, given]) * (1.0 / members)).astype(BF16)
    mean, first_rows = lax.optimization_barrier((mean, first_rows))
    mean = lax.all_to_all(mean, "space", split_axis=0, concat_axis=0, tiled=True)
    mean, rest = lax.optimization_barrier((mean, rest))
    last_rows = lax.all_to_all(rest, "space", split_axis=0, concat_axis=0, tiled=True)
    below = along_z(mean, 1)
    above = along_z(mean, 3)
    far_up = along_z(below[:, :1], 1)
    far_down = along_z(above[:, 1:], 3)
    other = [to_core(mean)]
    other.append(to_core(above))
    other += [to_core(far_up), to_core(far_down)]
    other.append(to_core(below))
    means = [mean, above, far_up, far_down, below, *other]

    groups = 7
    once = pl.Buffered(1)
    band = pl.BlockSpec((4 * groups, rows_local, lon_count), lambda i: (i, 0, 0))
    perturbed = pl.pallas_call(
        functools.partial(perturb_kernel, groups),
        grid=(channels // (4 * groups),),
        in_specs=[
            smem,
            smem,
            pl.BlockSpec(basis.shape, lambda i: (0, 0), pipeline_mode=once),
            band,
        ]
        + [pl.BlockSpec(x.shape, lambda i: (0, 0, 0, 0), pipeline_mode=once) for x in (first, rest, *means)],
        out_specs=band,
        out_shape=jax.ShapeDtypeStruct(weather.shape[1:], BF16),
        scratch_shapes=[pltpu.VMEM((bands, members, 128, 128), BF16)],
        compiler_params=pltpu.CompilerParams(vmem_limit_bytes=60 * 2**20),
        name="perturb",
    )(channel_scale, place, basis, weather[0], first_rows, last_rows, *means)
    return perturbed[None]


def solution(mesh):
    return jax.shard_map(
        local,
        mesh=mesh,
        in_specs=(P("member", None, "space", None), P("member", None, None, "space", None), P()),
        out_specs=P("member", None, "space", None),
        check_vma=False,
    )
```
